32 devices in a mesh: ctg: 8 (over y, x, core), br: 4 (over z).
Axes of the slice: x: 2, y: 2, z: 4, core: 2. Of those that a mesh axis runs over, the one named last changes fastest.
Arguments:
- base_vm: float32 [10240], P(('ctg', 'br')), may hold values from 0.95 to 1.05
- base_va: float32 [10240], P(('ctg', 'br')), may hold values from -0.6 to 0.6
- delta_state: float32 [64, 2, 10240], P('ctg', None, 'br'), may hold values from -0.18 to 0.18
- multipliers: float32 [64, 2, 10240], P('ctg', None, 'br'), may hold values from -6 to 6
- net_inj: float32 [64, 2, 10240], P('ctg', None, 'br'), may hold values from -6 to 6
- ang_grad: float32 [64, 10240], P('ctg', 'br'), may hold values from -6 to 6
- from_bus: int32 [13312], P('br'), may hold values from 0 to 10239
- to_bus: int32 [13312], P('br'), may hold values from 0 to 10239
- status: int32 [64, 13312], P('ctg', 'br'), may hold values 0 or 1
- conduct: float32 [13312], P('br'), may hold values from 1 to 5
- suscept: float32 [13312], P('br'), may hold values from -15 to -5
- charging: float32 [13312], P('br'), may hold values from 0.1 to 0.6
- rating: float32 [13312], P('br'), may hold values from 1 to 3
- slack: float32 [64, 13312], P('ctg', 'br'), may hold values from 0.05 to 2
- zdual: float32 [64, 13312], P('ctg', 'br'), may hold values from 0.05 to 2
Outputs:
- mismatch: float32 [64, 2, 10240], P('ctg', None, 'br')
- dual_res: float32 [64, 10240], P('ctg', 'br')
- limit_res: float32 [64, 13312], P('ctg', 'br')
- ctg_norms: float32 [64, 4], P('ctg')
- total_norms: float32 [4], replicated
The draws below stay inside these ranges and needn't reach their ends.
All inputs are finite; a program needn't handle non-finite values. No bound on the sum of `status` on one device may be relied on, other than what follows from the above.
Results may differ from the reference program's by a relative error of at most 0.0003.
Values sent between devices are 32-bit elements; how exact they have to be, the bound alone decides.
A program may use at most 64 MiB of HBM per device.

```python
import math
import jax
import jax.numpy as jnp
from jax import lax

NB = 10240
NL = 13312
CTG = 64


def place_ends(drawn, rng, smallest, high):
    longest = drawn.shape.index(max(drawn.shape))
    spots = []
    for shift in (0, 1):
        where = [jax.random.randint(jax.random.fold_in(rng, axis), (), 0, length) for axis, length in enumerate(drawn.shape)]
        where[longest] = (where[longest] + shift) % drawn.shape[longest]
        spots.append(tuple(where))
    return drawn.at[spots[0]].set(smallest).at[spots[1]].set(high)


def shard_levels(key, extent, shards, low, top_value):
    def one(position, shards_of):
        draws = jax.random.uniform(jax.random.fold_in(jax.random.fold_in(key, 6), position), (shards_of,), jnp.float32, low / len(shards), top_value / len(shards))
        return jnp.repeat(jnp.exp(draws), extent[position] // shards_of).reshape((-1,) + (1,) * (len(extent) - position - 1))

    loudness = one(*shards[0])
    for cut in shards[1:]:
        loudness = loudness * one(*cut)
    return loudness


def gaussian(key, extent, width, limit, split=(), dtype=jnp.bfloat16):
    array = jax.random.normal(key, extent, jnp.float32) * width
    if len(split) > 0:
        array = shard_levels(key, extent, split, -0.22, 0.18) * array
    return jnp.clip(array, min=-limit, max=limit).astype(dtype)


def setup_inputs(seed: int = 0) -> dict:
    streams_of = jax.random.split(jax.random.key(seed), 16)
    base_vm = jnp.clip(0.95 + 0.099999964 * jax.random.uniform(streams_of[0], (NB,), jnp.float32) ** shard_levels(streams_of[0], (NB,), ((0, 32),), -0.2, 0.2), 0.95, 1.05)
    base_va = gaussian(streams_of[1], (NB,), 0.1, 0.6, ((0, 32),), jnp.float32)
    delta_state = gaussian(streams_of[2], (CTG, 2, NB), 0.03, 0.18, ((0, 8), (2, 4)), jnp.float32)
    multipliers = gaussian(streams_of[3], (CTG, 2, NB), 1.0, 6.0, ((0, 8), (2, 4)), jnp.float32)
    net_inj = gaussian(streams_of[4], (CTG, 2, NB), 1.0, 6.0, ((0, 8), (2, 4)), jnp.float32)
    ang_grad = gaussian(streams_of[5], (CTG, NB), 1.0, 6.0, ((0, 8), (1, 4)), jnp.float32)
    from_bus = place_ends(jax.random.randint(streams_of[6], (NL,), 0, NB), jax.random.fold_in(streams_of[6], 1), 0, NB - 1).astype(jnp.int32)
    to_bus = place_ends(jax.random.randint(streams_of[7], (NL,), 0, NB), jax.random.fold_in(streams_of[7], 1), 0, NB - 1).astype(jnp.int32)
    status = place_ends((jax.random.randint(streams_of[8], (CTG, NL), 0, 8) < 7).astype(jnp.int32), jax.random.fold_in(streams_of[8], 1), 0, 1)
    conduct = jnp.clip(1.0 + 4.0 * jax.random.uniform(streams_of[9], (NL,), jnp.float32) ** shard_levels(streams_of[9], (NL,), ((0, 4),), -0.2, 0.2), 1.0, 5.0)
    suscept = jnp.clip(-15.0 + 10.0 * jax.random.uniform(streams_of[10], (NL,), jnp.float32) ** shard_levels(streams_of[10], (NL,), ((0, 4),), -0.2, 0.2), -15.0, -5.0)
    charging = jnp.clip(0.1 + 0.5 * jax.random.uniform(streams_of[11], (NL,), jnp.float32) ** shard_levels(streams_of[11], (NL,), ((0, 4),), -0.2, 0.2), 0.1, 0.6)
    rating = jnp.clip(1.0 + 2.0 * jax.random.uniform(streams_of[12], (NL,), jnp.float32) ** shard_levels(streams_of[12], (NL,), ((0, 4),), -0.2, 0.2), 1.0, 3.0)
    slack = jnp.clip(jnp.exp(math.log(2.0) - 3.6888794 * jax.random.uniform(streams_of[13], (CTG, NL), jnp.float32) ** shard_levels(streams_of[13], (CTG, NL), ((0, 8), (1, 4)), -0.2, 0.2)), 0.05, 2.0)
    zdual = jnp.clip(jnp.exp(math.log(2.0) - 3.6888794 * jax.random.uniform(streams_of[14], (CTG, NL), jnp.float32) ** shard_levels(streams_of[14], (CTG, NL), ((0, 8), (1, 4)), -0.2, 0.2)), 0.05, 2.0)
    return dict(base_vm=base_vm, base_va=base_va, delta_state=delta_state, multipliers=multipliers, net_inj=net_inj, ang_grad=ang_grad, from_bus=from_bus, to_bus=to_bus, status=status, conduct=conduct, suscept=suscept, charging=charging, rating=rating, slack=slack, zdual=zdual)


def branch_flows(volt_mag, volt_ang, mult_p, mult_q, from_idx, to_idx, conduct, suscept, charging, in_service):
    volt_from = volt_mag[:, from_idx]
    volt_to = volt_mag[:, to_idx]
    angle_diff = volt_ang[:, from_idx] - volt_ang[:, to_idx]
    cos_diff = jnp.cos(angle_diff)
    sin_diff = jnp.sin(angle_diff)
    volt_prod = volt_from * volt_to
    p_from = conduct * volt_from * volt_from - volt_prod * (conduct * cos_diff + suscept * sin_diff)
    q_from = -(suscept + charging) * volt_from * volt_from - volt_prod * (conduct * sin_diff - suscept * cos_diff)
    p_to = conduct * volt_to * volt_to - volt_prod * (conduct * cos_diff - suscept * sin_diff)
    q_to = -(suscept + charging) * volt_to * volt_to + volt_prod * (conduct * sin_diff + suscept * cos_diff)
    flow_dual = volt_prod * (mult_p[:, from_idx] * (conduct * sin_diff - suscept * cos_diff) - mult_q[:, from_idx] * (conduct * cos_diff + suscept * sin_diff) + mult_p[:, to_idx] * (conduct * sin_diff + suscept * cos_diff) + mult_q[:, to_idx] * (conduct * cos_diff - suscept * sin_diff))
    at_from = jnp.stack([p_from, q_from, flow_dual], 1) * in_service[:, None, :]
    at_to = jnp.stack([p_to, q_to, -flow_dual], 1) * in_service[:, None, :]
    return (at_from, at_to)

def reference(base_vm, base_va, delta_state, multipliers, net_inj, ang_grad, from_bus, to_bus, status, conduct, suscept, charging, rating, slack, zdual):
    volt_mag = base_vm[None, :] + delta_state[:, 0]
    volt_ang = base_va[None, :] + delta_state[:, 1]
    in_service = status.astype(jnp.float32)
    at_from, at_to = branch_flows(volt_mag, volt_ang, multipliers[:, 0], multipliers[:, 1], from_bus, to_bus, conduct, suscept, charging, in_service)
    scenarios = delta_state.shape[0]
    buses = delta_state.shape[2]
    summed = jnp.zeros((scenarios, 3, buses), jnp.float32)
    summed = summed.at[:, :, from_bus].add(at_from).at[:, :, to_bus].add(at_to)
    mismatch = summed[:, :2] - net_inj
    dual_res = summed[:, 2] + ang_grad
    limit_res = in_service * (at_from[:, 0] * at_from[:, 0] + at_from[:, 1] * at_from[:, 1] + slack - rating * rating)
    complement = in_service * (zdual * slack - 0.01)
    squares = jnp.stack([lax.optimization_barrier(jnp.sum(mismatch * mismatch, axis=(1, 2))), lax.optimization_barrier(jnp.sum(dual_res * dual_res, axis=1)), lax.optimization_barrier(jnp.sum(limit_res * limit_res, axis=1)), lax.optimization_barrier(jnp.sum(complement * complement, axis=1))], 1)
    ctg_norms = jnp.sqrt(squares)
    total_norms = jnp.sqrt(lax.optimization_barrier(jnp.sum(squares, axis=0)) / scenarios)
    return (mismatch, dual_res, limit_res, ctg_norms, total_norms)
```

```python
import functools

import jax
import jax.numpy as jnp
from jax import lax
from jax.experimental import pallas as pl
from jax.experimental.pallas import tpu as pltpu
from jax.sharding import PartitionSpec as P

LANES = 128
SPAN = 256
ROWS = 8
MESH = pl.DeviceIdType.MESH


def sin_cos(x):
    y = x * x
    sin_c = (1 / 6227020800, -1 / 39916800, 1 / 362880, -1 / 5040, 1 / 120, -1 / 6)
    cos_c = (-1 / 87178291200, 1 / 479001600, -1 / 3628800, 1 / 40320, -1 / 720, 1 / 24, -0.5)
    s = jnp.full_like(y, sin_c[0])
    for c in sin_c[1:]:
        s = s * y + c
    k = jnp.full_like(y, cos_c[0])
    for c in cos_c[1:]:
        k = k * y + c
    return x + x * y * s, 1.0 + y * k


def body(
    groups, ranks,
    base, delta, mult, net, ang, ends, params, rating, status3, status, slack, zdual,
    mis_out, dual_out, lim_out, norm_out, tot_out,
    dbuf, mbuf, ebuf, pbuf, stbuf, table, got, vals, left, onehot, acc,
    res, rbuf, flow, rflow, sqs, sqbuf,
    send, recv, sq_send, sq_recv,
):
    grp, me = lax.axis_index("ctg"), lax.axis_index("br")
    count = groups * ranks
    mine = grp * ranks + me
    per = dbuf.shape[1]
    nb, nl = delta.shape[2], ends.shape[1]
    scen = delta.shape[0]

    barrier = pltpu.get_barrier_semaphore()

    def greet(i, carry):
        peer = lax.rem(mine + i, count)
        pl.semaphore_signal(
            barrier, inc=1, device_id=(peer // ranks, lax.rem(peer, ranks)), device_id_type=MESH
        )
        return carry

    lax.fori_loop(1, count, greet, 0)
    pl.semaphore_wait(barrier, count - 1)

    def remote(src, dst, kind, step):
        return pltpu.make_async_remote_copy(
            src_ref=src, dst_ref=dst, send_sem=send.at[kind, step], recv_sem=recv.at[kind, step],
            device_id=(grp, lax.rem(me + step, ranks)), device_id_type=MESH,
        )

    first = []
    for step in range(1, ranks):
        peer = lax.rem(me + step, ranks)
        part = pl.ds(peer * per, per)
        first.append((
            remote(delta.at[part], dbuf.at[me], 0, step),
            remote(mult.at[part], mbuf.at[me], 1, step),
            remote(ends, ebuf.at[me], 2, step),
            remote(params, pbuf.at[me], 3, step),
            remote(status3.at[peer], stbuf.at[me], 4, step),
        ))
    for kind in range(5):
        for group in first:
            group[kind].start()

    own = pl.ds(me * per, per)
    dbuf[me] = delta[own]
    mbuf[me] = mult[own]
    ebuf[me] = ends[...]
    pbuf[me] = params[...]
    stbuf[me] = status3[me]
    table[...] = jnp.zeros_like(table)
    vals[...] = jnp.zeros_like(vals)
    acc[...] = jnp.zeros_like(acc)
    sqs[...] = jnp.zeros_like(sqs)
    live_own = status[...].astype(jnp.float32)
    comp = live_own * (zdual[...] * slack[...] - 0.01)
    sqs[:, 3:4] = jnp.sum(comp * comp, axis=1, keepdims=True)

    for group in first:
        for copy in group:
            copy.wait()

    for src in range(ranks):
        cols = slice(src * nb, (src + 1) * nb)
        for s in range(per):
            table[s : s + 1, cols] = base[0:1, cols] + dbuf[src, s, 0:1, :]
            table[per + s : per + s + 1, cols] = base[1:2, cols] + dbuf[src, s, 1:2, :]
            table[2 * per + s : 2 * per + s + 1, cols] = mbuf[src, s, 0:1, :]
            table[3 * per + s : 3 * per + s + 1, cols] = mbuf[src, s, 1:2, :]

    tiles = table.shape[1] // LANES
    high = table.shape[1] // SPAN

    def one_source(src, carry):
        def pick(t, c):
            cols = pl.ds(pl.multiple_of(t * LANES, LANES), LANES)
            for end in range(2):
                spot = jnp.broadcast_to(ebuf[src, end : end + 1, cols], (ROWS, LANES))
                low, tile = spot & (LANES - 1), spot >> 7
                found = jnp.zeros((ROWS, LANES), jnp.float32)
                for k in range(tiles):
                    piece = jnp.take_along_axis(
                        table[:, k * LANES : (k + 1) * LANES], low, axis=1, mode="promise_in_bounds"
                    )
                    found = jnp.where(tile == k, piece, found)
                got[end, :, cols] = found
            return c

        lax.fori_loop(0, nl // LANES, pick, 0)

        def quantity(end, q):
            return got[end, q * per : (q + 1) * per, :]

        vf, vt = quantity(0, 0), quantity(1, 0)
        sn, cs = sin_cos(quantity(0, 1) - quantity(1, 1))
        par = pbuf[src]
        g, b, h = par[0:1], par[1:2], par[2:3]
        live = stbuf[src].astype(jnp.float32)
        u = vf * vt
        gc_bs, gc_mbs = g * cs + b * sn, g * cs - b * sn
        gs_bc, gs_mbc = g * sn + b * cs, g * sn - b * cs
        bh = -(b + h)
        pf = live * (g * vf * vf - u * gc_bs)
        qf = live * (bh * vf * vf - u * gs_mbc)
        pt = live * (g * vt * vt - u * gc_mbs)
        qt = live * (bh * vt * vt + u * gs_bc)
        fd = live * u * (
            quantity(0, 2) * gs_mbc - quantity(0, 3) * gc_bs
            + quantity(1, 2) * gs_bc + quantity(1, 3) * gc_mbs
        )
        flow[src] = pf * pf + qf * qf
        vals[0, 0:per, :] = pf
        vals[0, per : 2 * per, :] = qf
        vals[0, 2 * per : 3 * per, :] = fd
        vals[1, 0:per, :] = pt
        vals[1, per : 2 * per, :] = qt
        vals[1, 2 * per : 3 * per, :] = -fd

        for end in range(2):
            def spread(t, c):
                cols = pl.ds(pl.multiple_of(t * LANES, LANES), LANES)
                spot = ebuf[src, end : end + 1, cols]
                low = jnp.broadcast_to(spot & (SPAN - 1), (SPAN, LANES))
                label = lax.broadcasted_iota(jnp.int32, (SPAN, LANES), 0)
                onehot[:, cols] = jnp.where(low == label, 1.0, 0.0).astype(jnp.bfloat16)
                row = jnp.broadcast_to(spot >> 8, (2 * ROWS, LANES))
                value = vals[end, :, cols]
                head = value.astype(jnp.bfloat16).astype(jnp.float32)
                both = jnp.concatenate([head, value - head], axis=0)
                for k in range(high):
                    left[k * 2 * ROWS : (k + 1) * 2 * ROWS, cols] = jnp.where(
                        row == k, both, 0.0
                    ).astype(jnp.bfloat16)
                return c

            lax.fori_loop(0, nl // LANES, spread, 0)
            acc[...] += lax.dot_general(
                left[...], onehot[...], (((1,), (1,)), ((), ())),
                preferred_element_type=jnp.float32,
            )
        return carry

    lax.fori_loop(0, ranks, one_source, 0)

    for k in range(high):
        at = k * SPAN
        row = k * 2 * ROWS
        res[at // nb, :, at % nb : at % nb + SPAN] = (
            acc[row : row + ROWS, :] + acc[row + ROWS : row + 2 * ROWS, :]
        )

    back = []
    for step in range(1, ranks):
        peer = lax.rem(me + step, ranks)
        back.append((
            remote(res.at[peer], rbuf.at[me], 5, step),
            remote(flow.at[peer], rflow.at[me], 6, step),
        ))
    for kind in range(2):
        for group in back:
            group[kind].start()
    rbuf[me] = res[me]
    rflow[me] = flow[me]
    for group in back:
        for copy in group:
            copy.wait()

    rate = rating[...] * rating[...]
    for src in range(ranks):
        sums = rbuf[src]
        for s in range(per):
            c = src * per + s
            total = jnp.zeros((1, 1), jnp.float32)
            for k in range(2):
                row = sums[k * per + s : k * per + s + 1, :] - net[c, k : k + 1, :]
                mis_out[c, k : k + 1, :] = row
                total = total + jnp.sum(row * row, axis=1, keepdims=True)
            sqs[c : c + 1, 0:1] = total
        rows = slice(src * per, (src + 1) * per)
        dual = sums[2 * per : 3 * per, :] + ang[rows, :]
        dual_out[rows, :] = dual
        sqs[rows, 1:2] = jnp.sum(dual * dual, axis=1, keepdims=True)
        lim = status[rows, :].astype(jnp.float32) * (rflow[src] + slack[rows, :] - rate)
        lim_out[rows, :] = lim
        sqs[rows, 2:3] = jnp.sum(lim * lim, axis=1, keepdims=True)

    sqbuf[mine] = sqs[...]

    def share(i):
        peer = lax.rem(mine + i, count)
        return pltpu.make_async_remote_copy(
            src_ref=sqbuf.at[mine], dst_ref=sqbuf.at[mine],
            send_sem=sq_send.at[i], recv_sem=sq_recv.at[i],
            device_id=(peer // ranks, lax.rem(peer, ranks)), device_id_type=MESH,
        )

    def begin(i, c):
        share(i).start()
        return c

    def finish(i, c):
        share(i).wait()
        return c

    lax.fori_loop(1, count, begin, 0)
    lax.fori_loop(1, count, finish, 0)

    def add(i, c):
        return c + sqbuf[i]

    zero = jnp.zeros((scen, LANES), jnp.float32)
    group_sum = zero
    for z in range(ranks):
        group_sum = group_sum + sqbuf[grp * ranks + z]
    norm_out[...] = jnp.sqrt(group_sum[:, 0:4])
    everything = jnp.sum(lax.fori_loop(0, count, add, zero), axis=0, keepdims=True)
    tot_out[...] = jnp.sqrt(everything[:, 0:4] / (scen * groups))


def per_device(
    base_vm, base_va, delta_state, multipliers, net_inj, ang_grad, from_bus, to_bus,
    status, conduct, suscept, charging, rating, slack, zdual,
):
    groups, ranks = lax.axis_size("ctg"), lax.axis_size("br")
    count = groups * ranks
    scen, _, nb = delta_state.shape
    nl = from_bus.shape[0]
    per = scen // ranks
    buses = nb * ranks
    high = buses // SPAN
    base = lax.all_gather(jnp.stack([base_vm, base_va]), ("ctg", "br"), axis=1, tiled=True)
    ends = jnp.stack([from_bus, to_bus])
    params = jnp.stack([conduct, suscept, charging])
    f32 = jnp.float32
    vmem = pl.BlockSpec(memory_space=pltpu.VMEM)
    mis, dual, lim, norms, tot = pl.pallas_call(
        functools.partial(body, groups, ranks),
        out_shape=(
            jax.ShapeDtypeStruct((scen, 2, nb), f32),
            jax.ShapeDtypeStruct((scen, nb), f32),
            jax.ShapeDtypeStruct((scen, nl), f32),
            jax.ShapeDtypeStruct((scen, 4), f32),
            jax.ShapeDtypeStruct((1, 4), f32),
        ),
        in_specs=[vmem] * 12,
        out_specs=(vmem,) * 5,
        scratch_shapes=[
            pltpu.VMEM((ranks, per, 2, nb), f32),
            pltpu.VMEM((ranks, per, 2, nb), f32),
            pltpu.VMEM((ranks, 2, nl), jnp.int32),
            pltpu.VMEM((ranks, 3, nl), f32),
            pltpu.VMEM((ranks, per, nl), jnp.int32),
            pltpu.VMEM((ROWS, buses), f32),
            pltpu.VMEM((2, ROWS, nl), f32),
            pltpu.VMEM((2, ROWS, nl), f32),
            pltpu.VMEM((high * 2 * ROWS, nl), jnp.bfloat16),
            pltpu.VMEM((SPAN, nl), jnp.bfloat16),
            pltpu.VMEM((high * 2 * ROWS, SPAN), f32),
            pltpu.VMEM((ranks, ROWS, nb), f32),
            pltpu.VMEM((ranks, ROWS, nb), f32),
            pltpu.VMEM((ranks, per, nl), f32),
            pltpu.VMEM((ranks, per, nl), f32),
            pltpu.VMEM((scen, LANES), f32),
            pltpu.VMEM((count, scen, LANES), f32),
            pltpu.SemaphoreType.DMA((7, ranks)),
            pltpu.SemaphoreType.DMA((7, ranks)),
            pltpu.SemaphoreType.DMA((count,)),
            pltpu.SemaphoreType.DMA((count,)),
        ],
        compiler_params=pltpu.CompilerParams(
            collective_id=0, has_side_effects=True, vmem_limit_bytes=48 << 20
        ),
    )(
        base, delta_state, multipliers, net_inj, ang_grad, ends, params, rating[None, :],
        status.reshape(ranks, per, nl), status, slack, zdual,
    )
    return (mis, dual, lim, norms, tot[0])


def solution(mesh):
    placed = (
        P(("ctg", "br")), P(("ctg", "br")),
        P("ctg", None, "br"), P("ctg", None, "br"), P("ctg", None, "br"), P("ctg", "br"),
        P("br"), P("br"), P("ctg", "br"), P("br"), P("br"), P("br"), P("br"),
        P("ctg", "br"), P("ctg", "br"),
    )
    return jax.shard_map(
        per_device,
        mesh=mesh,
        in_specs=placed,
        out_specs=(P("ctg", None, "br"), P("ctg", "br"), P("ctg", "br"), P("ctg", None), P()),
        check_vma=False,
    )
```

```python
import functools

import jax
import jax.numpy as jnp
from jax import lax
from jax.experimental import pallas as pl
from jax.experimental.pallas import tpu as pltpu
from jax.sharding import PartitionSpec as P

LANES = 128
SPAN = 256
ROWS = 8
MESH = pl.DeviceIdType.MESH


def sin_cos(x):
    y = x * x
    sin_c = (1 / 6227020800, -1 / 39916800, 1 / 362880, -1 / 5040, 1 / 120, -1 / 6)
    cos_c = (-1 / 87178291200, 1 / 479001600, -1 / 3628800, 1 / 40320, -1 / 720, 1 / 24, -0.5)
    s = jnp.full_like(y, sin_c[0])
    for c in sin_c[1:]:
        s = s * y + c
    k = jnp.full_like(y, cos_c[0])
    for c in cos_c[1:]:
        k = k * y + c
    return x + x * y * s, 1.0 + y * k


def body(
    groups, ranks,
    base, delta, mult, net, ang, ends, params, rating, status3, status, slack, zdual,
    mis_out, dual_out, lim_out, norm_out, tot_out,
    bbuf, dbuf, mbuf, ebuf, pbuf, stbuf, table, got, vals, left, onehot, acc,
    res, rbuf, flow, rflow, sqs, sqbuf,
    send, recv, base_send, base_recv, sq_send, sq_recv,
):
    grp, me = lax.axis_index("ctg"), lax.axis_index("br")
    count = groups * ranks
    mine = grp * ranks + me
    per = dbuf.shape[1]
    nb, nl = delta.shape[2], ends.shape[1]
    scen = delta.shape[0]

    barrier = pltpu.get_barrier_semaphore()

    def greet(i, carry):
        peer = lax.rem(mine + i, count)
        pl.semaphore_signal(
            barrier, inc=1, device_id=(peer // ranks, lax.rem(peer, ranks)), device_id_type=MESH
        )
        return carry

    lax.fori_loop(1, count, greet, 0)
    pl.semaphore_wait(barrier, count - 1)

    def remote(src, dst, kind, step):
        return pltpu.make_async_remote_copy(
            src_ref=src, dst_ref=dst, send_sem=send.at[kind, step], recv_sem=recv.at[kind, step],
            device_id=(grp, lax.rem(me + step, ranks)), device_id_type=MESH,
        )

    def all_peers(slots, block, sends, recvs, i):
        peer = lax.rem(mine + i, count)
        return pltpu.make_async_remote_copy(
            src_ref=block, dst_ref=slots.at[mine], send_sem=sends.at[i], recv_sem=recvs.at[i],
            device_id=(peer // ranks, lax.rem(peer, ranks)), device_id_type=MESH,
        )

    def begin_base(i, c):
        all_peers(bbuf, base, base_send, base_recv, i).start()
        return c

    def finish_base(i, c):
        all_peers(bbuf, base, base_send, base_recv, i).wait()
        return c

    lax.fori_loop(1, count, begin_base, 0)
    first = []
    for step in range(1, ranks):
        peer = lax.rem(me + step, ranks)
        part = pl.ds(peer * per, per)
        first.append((
            remote(delta.at[part], dbuf.at[me], 0, step),
            remote(mult.at[part], mbuf.at[me], 1, step),
            remote(ends, ebuf.at[me], 2, step),
            remote(params, pbuf.at[me], 3, step),
            remote(status3.at[peer], stbuf.at[me], 4, step),
        ))
    for kind in range(5):
        for group in first:
            group[kind].start()

    own = pl.ds(me * per, per)
    bbuf[mine] = base[...]
    dbuf[me] = delta[own]
    mbuf[me] = mult[own]
    ebuf[me] = ends[...]
    pbuf[me] = params[...]
    stbuf[me] = status3[me]
    table[...] = jnp.zeros_like(table)
    vals[...] = jnp.zeros_like(vals)
    acc[...] = jnp.zeros_like(acc)
    sqs[...] = jnp.zeros_like(sqs)
    live_own = status[...].astype(jnp.float32)
    comp = live_own * (zdual[...] * slack[...] - 0.01)
    sqs[:, 3:4] = jnp.sum(comp * comp, axis=1, keepdims=True)

    lax.fori_loop(1, count, finish_base, 0)
    for group in first:
        for copy in group:
            copy.wait()

    for src in range(ranks):
        cols = slice(src * nb, (src + 1) * nb)
        volts = jnp.concatenate([bbuf[src * groups + i] for i in range(groups)], axis=1)
        for s in range(per):
            table[s : s + 1, cols] = volts[0:1] + dbuf[src, s, 0:1, :]
            table[per + s : per + s + 1, cols] = volts[1:2] + dbuf[src, s, 1:2, :]
            table[2 * per + s : 2 * per + s + 1, cols] = mbuf[src, s, 0:1, :]
            table[3 * per + s : 3 * per + s + 1, cols] = mbuf[src, s, 1:2, :]

    tiles = table.shape[1] // LANES
    high = table.shape[1] // SPAN

    def one_source(src, carry):
        def pick(t, c):
            cols = pl.ds(pl.multiple_of(t * LANES, LANES), LANES)
            for end in range(2):
                spot = jnp.broadcast_to(ebuf[src, end : end + 1, cols], (ROWS, LANES))
                low, tile = spot & (LANES - 1), spot >> 7
                found = jnp.zeros((ROWS, LANES), jnp.float32)
                for k in range(tiles):
                    piece = jnp.take_along_axis(
                        table[:, k * LANES : (k + 1) * LANES], low, axis=1, mode="promise_in_bounds"
                    )
                    found = jnp.where(tile == k, piece, found)
                got[end, :, cols] = found
            return c

        lax.fori_loop(0, nl // LANES, pick, 0)

        def quantity(end, q):
            return got[end, q * per : (q + 1) * per, :]

        vf, vt = quantity(0, 0), quantity(1, 0)
        sn, cs = sin_cos(quantity(0, 1) - quantity(1, 1))
        par = pbuf[src]
        g, b, h = par[0:1], par[1:2], par[2:3]
        live = stbuf[src].astype(jnp.float32)
        u = vf * vt
        gc_bs, gc_mbs = g * cs + b * sn, g * cs - b * sn
        gs_bc, gs_mbc = g * sn + b * cs, g * sn - b * cs
        bh = -(b + h)
        pf = live * (g * vf * vf - u * gc_bs)
        qf = live * (bh * vf * vf - u * gs_mbc)
        pt = live * (g * vt * vt - u * gc_mbs)
        qt = live * (bh * vt * vt + u * gs_bc)
        fd = live * u * (
            quantity(0, 2) * gs_mbc - quantity(0, 3) * gc_bs
            + quantity(1, 2) * gs_bc + quantity(1, 3) * gc_mbs
        )
        flow[src] = pf * pf + qf * qf
        vals[0, 0:per, :] = pf
        vals[0, per : 2 * per, :] = qf
        vals[0, 2 * per : 3 * per, :] = fd
        vals[1, 0:per, :] = pt
        vals[1, per : 2 * per, :] = qt
        vals[1, 2 * per : 3 * per, :] = -fd

        for end in range(2):
            def spread(t, c):
                cols = pl.ds(pl.multiple_of(t * LANES, LANES), LANES)
                spot = ebuf[src, end : end + 1, cols]
                low = jnp.broadcast_to(spot & (SPAN - 1), (SPAN, LANES))
                label = lax.broadcasted_iota(jnp.int32, (SPAN, LANES), 0)
                onehot[:, cols] = jnp.where(low == label, 1.0, 0.0).astype(jnp.bfloat16)
                row = jnp.broadcast_to(spot >> 8, (2 * ROWS, LANES))
                value = vals[end, :, cols]
                head = value.astype(jnp.bfloat16).astype(jnp.float32)
                both = jnp.concatenate([head, value - head], axis=0)
                for k in range(high):
                    left[k * 2 * ROWS : (k + 1) * 2 * ROWS, cols] = jnp.where(
                        row == k, both, 0.0
                    ).astype(jnp.bfloat16)
                return c

            lax.fori_loop(0, nl // LANES, spread, 0)
            acc[...] += lax.dot_general(
                left[...], onehot[...], (((1,), (1,)), ((), ())),
                preferred_element_type=jnp.float32,
            )
        return carry

    lax.fori_loop(0, ranks, one_source, 0)

    for k in range(high):
        at = k * SPAN
        row = k * 2 * ROWS
        res[at // nb, :, at % nb : at % nb + SPAN] = (
            acc[row : row + ROWS, :] + acc[row + ROWS : row + 2 * ROWS, :]
        )

    back = []
    for step in range(1, ranks):
        peer = lax.rem(me + step, ranks)
        back.append((
            remote(res.at[peer], rbuf.at[me], 5, step),
            remote(flow.at[peer], rflow.at[me], 6, step),
        ))
    for kind in range(2):
        for group in back:
            group[kind].start()
    rbuf[me] = res[me]
    rflow[me] = flow[me]
    for group in back:
        for copy in group:
            copy.wait()

    rate = rating[...] * rating[...]
    for src in range(ranks):
        sums = rbuf[src]
        for s in range(per):
            c = src * per + s
            total = jnp.zeros((1, 1), jnp.float32)
            for k in range(2):
                row = sums[k * per + s : k * per + s + 1, :] - net[c, k : k + 1, :]
                mis_out[c, k : k + 1, :] = row
                total = total + jnp.sum(row * row, axis=1, keepdims=True)
            sqs[c : c + 1, 0:1] = total
        rows = slice(src * per, (src + 1) * per)
        dual = sums[2 * per : 3 * per, :] + ang[rows, :]
        dual_out[rows, :] = dual
        sqs[rows, 1:2] = jnp.sum(dual * dual, axis=1, keepdims=True)
        lim = status[rows, :].astype(jnp.float32) * (rflow[src] + slack[rows, :] - rate)
        lim_out[rows, :] = lim
        sqs[rows, 2:3] = jnp.sum(lim * lim, axis=1, keepdims=True)

    sqbuf[mine] = sqs[...]

    def begin(i, c):
        all_peers(sqbuf, sqbuf.at[mine], sq_send, sq_recv, i).start()
        return c

    def finish(i, c):
        all_peers(sqbuf, sqbuf.at[mine], sq_send, sq_recv, i).wait()
        return c

    lax.fori_loop(1, count, begin, 0)
    lax.fori_loop(1, count, finish, 0)

    def add(i, c):
        return c + sqbuf[i]

    zero = jnp.zeros((scen, LANES), jnp.float32)
    group_sum = zero
    for z in range(ranks):
        group_sum = group_sum + sqbuf[grp * ranks + z]
    norm_out[...] = jnp.sqrt(group_sum[:, 0:4])
    everything = jnp.sum(lax.fori_loop(0, count, add, zero), axis=0, keepdims=True)
    tot_out[...] = jnp.sqrt(everything[:, 0:4] / (scen * groups))


def per_device(
    base_vm, base_va, delta_state, multipliers, net_inj, ang_grad, from_bus, to_bus,
    status, conduct, suscept, charging, rating, slack, zdual,
):
    groups, ranks = lax.axis_size("ctg"), lax.axis_size("br")
    count = groups * ranks
    scen, _, nb = delta_state.shape
    nl = from_bus.shape[0]
    per = scen // ranks
    buses = nb * ranks
    high = buses // SPAN
    base = jnp.stack([base_vm, base_va])
    ends = jnp.stack([from_bus, to_bus])
    params = jnp.stack([conduct, suscept, charging])
    f32 = jnp.float32
    vmem = pl.BlockSpec(memory_space=pltpu.VMEM)
    mis, dual, lim, norms, tot = pl.pallas_call(
        functools.partial(body, groups, ranks),
        out_shape=(
            jax.ShapeDtypeStruct((scen, 2, nb), f32),
            jax.ShapeDtypeStruct((scen, nb), f32),
            jax.ShapeDtypeStruct((scen, nl), f32),
            jax.ShapeDtypeStruct((scen, 4), f32),
            jax.ShapeDtypeStruct((1, 4), f32),
        ),
        in_specs=[vmem] * 12,
        out_specs=(vmem,) * 5,
        scratch_shapes=[
            pltpu.VMEM((count, 2, base_vm.shape[0]), f32),
            pltpu.VMEM((ranks, per, 2, nb), f32),
            pltpu.VMEM((ranks, per, 2, nb), f32),
            pltpu.VMEM((ranks, 2, nl), jnp.int32),
            pltpu.VMEM((ranks, 3, nl), f32),
            pltpu.VMEM((ranks, per, nl), jnp.int32),
            pltpu.VMEM((ROWS, buses), f32),
            pltpu.VMEM((2, ROWS, nl), f32),
            pltpu.VMEM((2, ROWS, nl), f32),
            pltpu.VMEM((high * 2 * ROWS, nl), jnp.bfloat16),
            pltpu.VMEM((SPAN, nl), jnp.bfloat16),
            pltpu.VMEM((high * 2 * ROWS, SPAN), f32),
            pltpu.VMEM((ranks, ROWS, nb), f32),
            pltpu.VMEM((ranks, ROWS, nb), f32),
            pltpu.VMEM((ranks, per, nl), f32),
            pltpu.VMEM((ranks, per, nl), f32),
            pltpu.VMEM((scen, LANES), f32),
            pltpu.VMEM((count, scen, LANES), f32),
            pltpu.SemaphoreType.DMA((7, ranks)),
            pltpu.SemaphoreType.DMA((7, ranks)),
            pltpu.SemaphoreType.DMA((count,)),
            pltpu.SemaphoreType.DMA((count,)),
            pltpu.SemaphoreType.DMA((count,)),
            pltpu.SemaphoreType.DMA((count,)),
        ],
        compiler_params=pltpu.CompilerParams(
            collective_id=0, has_side_effects=True, vmem_limit_bytes=48 << 20
        ),
    )(
        base, delta_state, multipliers, net_inj, ang_grad, ends, params, rating[None, :],
        status.reshape(ranks, per, nl), status, slack, zdual,
    )
    return (mis, dual, lim, norms, tot[0])


def solution(mesh):
    placed = (
        P(("ctg", "br")), P(("ctg", "br")),
        P("ctg", None, "br"), P("ctg", None, "br"), P("ctg", None, "br"), P("ctg", "br"),
        P("br"), P("br"), P("ctg", "br"), P("br"), P("br"), P("br"), P("br"),
        P("ctg", "br"), P("ctg", "br"),
    )
    return jax.shard_map(
        per_device,
        mesh=mesh,
        in_specs=placed,
        out_specs=(P("ctg", None, "br"), P("ctg", "br"), P("ctg", "br"), P("ctg", None), P()),
        check_vma=False,
    )
```

```python
import functools

import jax
import jax.numpy as jnp
from jax import lax
from jax.experimental import pallas as pl
from jax.experimental.pallas import tpu as pltpu
from jax.sharding import PartitionSpec as P

LANES = 128
SPAN = 256
ROWS = 8
MESH = pl.DeviceIdType.MESH


def sin_cos(x):
    y = x * x
    sin_c = (1 / 6227020800, -1 / 39916800, 1 / 362880, -1 / 5040, 1 / 120, -1 / 6)
    cos_c = (-1 / 87178291200, 1 / 479001600, -1 / 3628800, 1 / 40320, -1 / 720, 1 / 24, -0.5)
    s = jnp.full_like(y, sin_c[0])
    for c in sin_c[1:]:
        s = s * y + c
    k = jnp.full_like(y, cos_c[0])
    for c in cos_c[1:]:
        k = k * y + c
    return x + x * y * s, 1.0 + y * k


def body(
    groups, ranks,
    base, delta, mult, net, ang, ends, params, rating, status3, status, slack, zdual,
    mis_out, dual_out, lim_out, norm_out, tot_out,
    bbuf, dbuf, mbuf, ebuf, pbuf, stbuf, table, acc,
    res, rbuf, flow, rflow, sqs, sqbuf,
    send, recv, base_send, base_recv, sq_send, sq_recv,
):
    grp, me = lax.axis_index("ctg"), lax.axis_index("br")
    count = groups * ranks
    mine = grp * ranks + me
    per = dbuf.shape[1]
    nb, nl = delta.shape[2], ends.shape[1]
    scen = delta.shape[0]

    barrier = pltpu.get_barrier_semaphore()

    def greet(i, carry):
        peer = lax.rem(mine + i, count)
        pl.semaphore_signal(
            barrier, inc=1, device_id=(peer // ranks, lax.rem(peer, ranks)), device_id_type=MESH
        )
        return carry

    lax.fori_loop(1, count, greet, 0)
    pl.semaphore_wait(barrier, count - 1)

    def remote(src, dst, kind, step):
        return pltpu.make_async_remote_copy(
            src_ref=src, dst_ref=dst, send_sem=send.at[kind, step], recv_sem=recv.at[kind, step],
            device_id=(grp, lax.rem(me + step, ranks)), device_id_type=MESH,
        )

    def all_peers(slots, block, sends, recvs, i):
        peer = lax.rem(mine + i, count)
        return pltpu.make_async_remote_copy(
            src_ref=block, dst_ref=slots.at[mine], send_sem=sends.at[i], recv_sem=recvs.at[i],
            device_id=(peer // ranks, lax.rem(peer, ranks)), device_id_type=MESH,
        )

    def begin_base(i, c):
        all_peers(bbuf, base, base_send, base_recv, i).start()
        return c

    def finish_base(i, c):
        all_peers(bbuf, base, base_send, base_recv, i).wait()
        return c

    lax.fori_loop(1, count, begin_base, 0)
    first = []
    for step in range(1, ranks):
        peer = lax.rem(me + step, ranks)
        part = pl.ds(peer * per, per)
        first.append((
            remote(delta.at[part], dbuf.at[me], 0, step),
            remote(mult.at[part], mbuf.at[me], 1, step),
            remote(ends, ebuf.at[me], 2, step),
            remote(params, pbuf.at[me], 3, step),
            remote(status3.at[peer], stbuf.at[me], 4, step),
        ))
    for kind in range(5):
        for group in first:
            group[kind].start()

    own = pl.ds(me * per, per)
    bbuf[mine] = base[...]
    dbuf[me] = delta[own]
    mbuf[me] = mult[own]
    ebuf[me] = ends[...]
    pbuf[me] = params[...]
    stbuf[me] = status3[me]
    table[...] = jnp.zeros_like(table)
    acc[...] = jnp.zeros_like(acc)
    sqs[...] = jnp.zeros_like(sqs)
    live_own = status[...].astype(jnp.float32)
    comp = live_own * (zdual[...] * slack[...] - 0.01)
    sqs[:, 3:4] = jnp.sum(comp * comp, axis=1, keepdims=True)

    lax.fori_loop(1, count, finish_base, 0)
    for group in first:
        for copy in group:
            copy.wait()

    for src in range(ranks):
        cols = slice(src * nb, (src + 1) * nb)
        volts = jnp.concatenate([bbuf[src * groups + i] for i in range(groups)], axis=1)
        for s in range(per):
            table[s : s + 1, cols] = volts[0:1] + dbuf[src, s, 0:1, :]
            table[per + s : per + s + 1, cols] = volts[1:2] + dbuf[src, s, 1:2, :]
            table[2 * per + s : 2 * per + s + 1, cols] = mbuf[src, s, 0:1, :]
            table[3 * per + s : 3 * per + s + 1, cols] = mbuf[src, s, 1:2, :]

    tiles = table.shape[1] // LANES
    high = table.shape[1] // SPAN

    chunk = SPAN if nl % SPAN == 0 else LANES
    pieces = nl // chunk
    bf16 = jnp.bfloat16

    def place(i):
        return i // pieces, pl.ds(pl.multiple_of(lax.rem(i, pieces) * chunk, chunk), chunk)

    def pick(i):
        src, cols = place(i)
        picked = []
        for end in range(2):
            spots = jnp.broadcast_to(ebuf[src, end : end + 1, cols], (ROWS, chunk))
            tiles_found = []
            for at in range(0, chunk, LANES):
                spot = spots[:, at : at + LANES]
                low, tile = spot & (LANES - 1), spot >> 7
                found = jnp.zeros((ROWS, LANES), jnp.float32)
                for k in range(tiles):
                    piece = jnp.take_along_axis(
                        table[:, k * LANES : (k + 1) * LANES], low, axis=1, mode="promise_in_bounds"
                    )
                    found = jnp.where(tile == k, piece, found)
                tiles_found.append(found)
            picked.append(jnp.concatenate(tiles_found, axis=1))
        return tuple(picked)

    def process(i, picked):
        src, cols = place(i)

        def quantity(end, q):
            return picked[end][q * per : (q + 1) * per, :]

        vf, vt = quantity(0, 0), quantity(1, 0)
        sn, cs = sin_cos(quantity(0, 1) - quantity(1, 1))
        par = pbuf[src, :, cols]
        g, b, h = par[0:1], par[1:2], par[2:3]
        live = stbuf[src, :, cols].astype(jnp.float32)
        u = vf * vt
        gc_bs, gc_mbs = g * cs + b * sn, g * cs - b * sn
        gs_bc, gs_mbc = g * sn + b * cs, g * sn - b * cs
        bh = -(b + h)
        pf = live * (g * vf * vf - u * gc_bs)
        qf = live * (bh * vf * vf - u * gs_mbc)
        pt = live * (g * vt * vt - u * gc_mbs)
        qt = live * (bh * vt * vt + u * gs_bc)
        fd = live * u * (
            quantity(0, 2) * gs_mbc - quantity(0, 3) * gc_bs
            + quantity(1, 2) * gs_bc + quantity(1, 3) * gc_mbs
        )
        flow[src, :, cols] = pf * pf + qf * qf
        blank = [jnp.zeros((ROWS - 3 * per, chunk), jnp.float32)]
        lefts, hots = [], []
        label = lax.broadcasted_iota(jnp.int32, (SPAN, chunk), 0).astype(bf16)
        for end, terms in ((0, [pf, qf, fd]), (1, [pt, qt, -fd])):
            value = jnp.concatenate(terms + blank, axis=0)
            head = value.astype(bf16).astype(jnp.float32)
            both = jnp.concatenate([head, value - head], axis=0).astype(bf16)
            spot = ebuf[src, end : end + 1, cols]
            row = jnp.broadcast_to(spot >> 8, (2 * ROWS, chunk)).astype(bf16)
            low = jnp.broadcast_to((spot & (SPAN - 1)), (2 * ROWS, chunk)).astype(bf16)
            low = jnp.concatenate([low] * (SPAN // (2 * ROWS)), axis=0)
            hots.append(jnp.where(low == label, bf16(1), bf16(0)))
            lefts.append(jnp.concatenate(
                [jnp.where(row == bf16(k), both, bf16(0)) for k in range(high)], axis=0
            ))
        acc[...] += lax.dot_general(
            jnp.concatenate(lefts, axis=1), jnp.concatenate(hots, axis=1),
            (((1,), (1,)), ((), ())), preferred_element_type=jnp.float32,
        )

    def advance(i, picked):
        following = pick(i)
        process(i - 1, picked)
        return following

    last = lax.fori_loop(1, ranks * pieces, advance, pick(0))
    process(ranks * pieces - 1, last)

    for k in range(high):
        at = k * SPAN
        row = k * 2 * ROWS
        res[at // nb, :, at % nb : at % nb + SPAN] = (
            acc[row : row + ROWS, :] + acc[row + ROWS : row + 2 * ROWS, :]
        )

    back = []
    for step in range(1, ranks):
        peer = lax.rem(me + step, ranks)
        back.append((
            remote(res.at[peer], rbuf.at[me], 5, step),
            remote(flow.at[peer], rflow.at[me], 6, step),
        ))
    for kind in range(2):
        for group in back:
            group[kind].start()
    rbuf[me] = res[me]
    rflow[me] = flow[me]
    for group in back:
        for copy in group:
            copy.wait()

    rate = rating[...] * rating[...]
    for src in range(ranks):
        sums = rbuf[src]
        for s in range(per):
            c = src * per + s
            total = jnp.zeros((1, 1), jnp.float32)
            for k in range(2):
                row = sums[k * per + s : k * per + s + 1, :] - net[c, k : k + 1, :]
                mis_out[c, k : k + 1, :] = row
                total = total + jnp.sum(row * row, axis=1, keepdims=True)
            sqs[c : c + 1, 0:1] = total
        rows = slice(src * per, (src + 1) * per)
        dual = sums[2 * per : 3 * per, :] + ang[rows, :]
        dual_out[rows, :] = dual
        sqs[rows, 1:2] = jnp.sum(dual * dual, axis=1, keepdims=True)
        lim = status[rows, :].astype(jnp.float32) * (rflow[src] + slack[rows, :] - rate)
        lim_out[rows, :] = lim
        sqs[rows, 2:3] = jnp.sum(lim * lim, axis=1, keepdims=True)

    sqbuf[mine] = sqs[...]

    def begin(i, c):
        all_peers(sqbuf, sqbuf.at[mine], sq_send, sq_recv, i).start()
        return c

    def finish(i, c):
        all_peers(sqbuf, sqbuf.at[mine], sq_send, sq_recv, i).wait()
        return c

    lax.fori_loop(1, count, begin, 0)
    lax.fori_loop(1, count, finish, 0)

    def add(i, c):
        return c + sqbuf[i]

    zero = jnp.zeros((scen, LANES), jnp.float32)
    group_sum = zero
    for z in range(ranks):
        group_sum = group_sum + sqbuf[grp * ranks + z]
    norm_out[...] = jnp.sqrt(group_sum[:, 0:4])
    everything = jnp.sum(lax.fori_loop(0, count, add, zero), axis=0, keepdims=True)
    tot_out[...] = jnp.sqrt(everything[:, 0:4] / (scen * groups))


def per_device(
    base_vm, base_va, delta_state, multipliers, net_inj, ang_grad, from_bus, to_bus,
    status, conduct, suscept, charging, rating, slack, zdual,
):
    groups, ranks = lax.axis_size("ctg"), lax.axis_size("br")
    count = groups * ranks
    scen, _, nb = delta_state.shape
    nl = from_bus.shape[0]
    per = scen // ranks
    buses = nb * ranks
    high = buses // SPAN
    base = jnp.stack([base_vm, base_va])
    ends = jnp.stack([from_bus, to_bus])
    params = jnp.stack([conduct, suscept, charging])
    f32 = jnp.float32
    vmem = pl.BlockSpec(memory_space=pltpu.VMEM)
    mis, dual, lim, norms, tot = pl.pallas_call(
        functools.partial(body, groups, ranks),
        out_shape=(
            jax.ShapeDtypeStruct((scen, 2, nb), f32),
            jax.ShapeDtypeStruct((scen, nb), f32),
            jax.ShapeDtypeStruct((scen, nl), f32),
            jax.ShapeDtypeStruct((scen, 4), f32),
            jax.ShapeDtypeStruct((1, 4), f32),
        ),
        in_specs=[vmem] * 12,
        out_specs=(vmem,) * 5,
        scratch_shapes=[
            pltpu.VMEM((count, 2, base_vm.shape[0]), f32),
            pltpu.VMEM((ranks, per, 2, nb), f32),
            pltpu.VMEM((ranks, per, 2, nb), f32),
            pltpu.VMEM((ranks, 2, nl), jnp.int32),
            pltpu.VMEM((ranks, 3, nl), f32),
            pltpu.VMEM((ranks, per, nl), jnp.int32),
            pltpu.VMEM((ROWS, buses), f32),
            pltpu.VMEM((high * 2 * ROWS, SPAN), f32),
            pltpu.VMEM((ranks, ROWS, nb), f32),
            pltpu.VMEM((ranks, ROWS, nb), f32),
            pltpu.VMEM((ranks, per, nl), f32),
            pltpu.VMEM((ranks, per, nl), f32),
            pltpu.VMEM((scen, LANES), f32),
            pltpu.VMEM((count, scen, LANES), f32),
            pltpu.SemaphoreType.DMA((7, ranks)),
            pltpu.SemaphoreType.DMA((7, ranks)),
            pltpu.SemaphoreType.DMA((count,)),
            pltpu.SemaphoreType.DMA((count,)),
            pltpu.SemaphoreType.DMA((count,)),
            pltpu.SemaphoreType.DMA((count,)),
        ],
        compiler_params=pltpu.CompilerParams(
            collective_id=0, has_side_effects=True, vmem_limit_bytes=48 << 20
        ),
    )(
        base, delta_state, multipliers, net_inj, ang_grad, ends, params, rating[None, :],
        status.reshape(ranks, per, nl), status, slack, zdual,
    )
    return (mis, dual, lim, norms, tot[0])


def solution(mesh):
    placed = (
        P(("ctg", "br")), P(("ctg", "br")),
        P("ctg", None, "br"), P("ctg", None, "br"), P("ctg", None, "br"), P("ctg", "br"),
        P("br"), P("br"), P("ctg", "br"), P("br"), P("br"), P("br"), P("br"),
        P("ctg", "br"), P("ctg", "br"),
    )
    return jax.shard_map(
        per_device,
        mesh=mesh,
        in_specs=placed,
        out_specs=(P("ctg", None, "br"), P("ctg", "br"), P("ctg", "br"), P("ctg", None), P()),
        check_vma=False,
    )
```

```python
import functools

import jax
import jax.numpy as jnp
from jax import lax
from jax.experimental import pallas as pl
from jax.experimental.pallas import tpu as pltpu
from jax.sharding import PartitionSpec as P

LANES = 128
SPAN = 256
ROWS = 8
MESH = pl.DeviceIdType.MESH


def sin_cos(x):
    y = x * x
    sin_c = (1 / 6227020800, -1 / 39916800, 1 / 362880, -1 / 5040, 1 / 120, -1 / 6)
    cos_c = (-1 / 87178291200, 1 / 479001600, -1 / 3628800, 1 / 40320, -1 / 720, 1 / 24, -0.5)
    s = jnp.full_like(y, sin_c[0])
    for c in sin_c[1:]:
        s = s * y + c
    k = jnp.full_like(y, cos_c[0])
    for c in cos_c[1:]:
        k = k * y + c
    return x + x * y * s, 1.0 + y * k


def body(
    groups, ranks,
    base, delta, mult, net_any, ang_any, ends, params, rating, status3, status_any, slack_any, zdual_any,
    mis_out, dual_out, lim_out, norm_out, tot_out,
    bbuf, dbuf, mbuf, ebuf, pbuf, stbuf, table, acc,
    res, rbuf, flow, rflow, sqs, sqbuf, rowbuf,
    net, ang, status, slack, zdual, local,
    send, recv, base_send, base_recv, sq_send, sq_recv,
):
    grp, me = lax.axis_index("ctg"), lax.axis_index("br")
    count = groups * ranks
    mine = grp * ranks + me
    per = dbuf.shape[1]
    nb, nl = delta.shape[2], ends.shape[1]
    scen = delta.shape[0]

    own = pl.ds(me * per, per)
    local_copies = [
        pltpu.make_async_copy(a, b, local.at[i])
        for i, (a, b) in enumerate((
            (delta.at[own], dbuf.at[me]), (mult.at[own], mbuf.at[me]),
            (status_any, status), (slack_any, slack), (zdual_any, zdual),
            (net_any, net), (ang_any, ang),
        ))
    ]
    for copy in local_copies:
        copy.start()

    barrier = pltpu.get_barrier_semaphore()

    def greet(i, carry):
        peer = lax.rem(mine + i, count)
        pl.semaphore_signal(
            barrier, inc=1, device_id=(peer // ranks, lax.rem(peer, ranks)), device_id_type=MESH
        )
        return carry

    lax.fori_loop(1, count, greet, 0)
    pl.semaphore_wait(barrier, count - 1)

    def remote(src, dst, kind, step):
        return pltpu.make_async_remote_copy(
            src_ref=src, dst_ref=dst, send_sem=send.at[kind, step], recv_sem=recv.at[kind, step],
            device_id=(grp, lax.rem(me + step, ranks)), device_id_type=MESH,
        )

    def all_peers(slots, block, sends, recvs, i):
        peer = lax.rem(mine + i, count)
        return pltpu.make_async_remote_copy(
            src_ref=block, dst_ref=slots.at[mine], send_sem=sends.at[i], recv_sem=recvs.at[i],
            device_id=(peer // ranks, lax.rem(peer, ranks)), device_id_type=MESH,
        )

    def begin_base(i, c):
        all_peers(bbuf, base, base_send, base_recv, i).start()
        return c

    def finish_base(i, c):
        all_peers(bbuf, base, base_send, base_recv, i).wait()
        return c

    lax.fori_loop(1, count, begin_base, 0)
    first = []
    for step in range(1, ranks):
        peer = lax.rem(me + step, ranks)
        part = pl.ds(peer * per, per)
        first.append((
            remote(delta.at[part], dbuf.at[me], 0, step),
            remote(mult.at[part], mbuf.at[me], 1, step),
            remote(ends, ebuf.at[me], 2, step),
            remote(params, pbuf.at[me], 3, step),
            remote(status3.at[peer], stbuf.at[me], 4, step),
        ))
    for kind in range(5):
        for group in first:
            group[kind].start()

    bbuf[mine] = base[...]
    ebuf[me] = ends[...]
    pbuf[me] = params[...]
    stbuf[me] = status3[me]
    table[...] = jnp.zeros_like(table)
    acc[...] = jnp.zeros_like(acc)
    sqs[...] = jnp.zeros_like(sqs)
    for copy in local_copies:
        copy.wait()
    live_own = status[...].astype(jnp.float32)
    comp = live_own * (zdual[...] * slack[...] - 0.01)
    sqs[:, 3:4] = jnp.sum(comp * comp, axis=1, keepdims=True)

    lax.fori_loop(1, count, finish_base, 0)
    for group in first:
        for copy in group[:3]:
            copy.wait()

    for src in range(ranks):
        cols = slice(src * nb, (src + 1) * nb)
        volts = jnp.concatenate([bbuf[src * groups + i] for i in range(groups)], axis=1)
        for s in range(per):
            table[s : s + 1, cols] = volts[0:1] + dbuf[src, s, 0:1, :]
            table[per + s : per + s + 1, cols] = volts[1:2] + dbuf[src, s, 1:2, :]
            table[2 * per + s : 2 * per + s + 1, cols] = mbuf[src, s, 0:1, :]
            table[3 * per + s : 3 * per + s + 1, cols] = mbuf[src, s, 1:2, :]

    tiles = table.shape[1] // LANES
    high = table.shape[1] // SPAN

    chunk = SPAN if nl % SPAN == 0 else LANES
    pieces = nl // chunk
    bf16 = jnp.bfloat16

    def place(i):
        return lax.rem(me - i // pieces + ranks, ranks), pl.ds(pl.multiple_of(lax.rem(i, pieces) * chunk, chunk), chunk)

    def pick(i):
        src, cols = place(i)
        picked = []
        for end in range(2):
            spots = jnp.broadcast_to(ebuf[src, end : end + 1, cols], (ROWS, chunk))
            tiles_found = []
            for at in range(0, chunk, LANES):
                spot = spots[:, at : at + LANES]
                low, tile = spot & (LANES - 1), spot >> 7
                found = jnp.zeros((ROWS, LANES), jnp.float32)
                for k in range(tiles):
                    piece = jnp.take_along_axis(
                        table[:, k * LANES : (k + 1) * LANES], low, axis=1, mode="promise_in_bounds"
                    )
                    found = jnp.where(tile == k, piece, found)
                tiles_found.append(found)
            picked.append(jnp.concatenate(tiles_found, axis=1))
        return tuple(picked)

    def process(i, picked):
        src, cols = place(i)

        def quantity(end, q):
            return picked[end][q * per : (q + 1) * per, :]

        vf, vt = quantity(0, 0), quantity(1, 0)
        sn, cs = sin_cos(quantity(0, 1) - quantity(1, 1))
        par = pbuf[src, :, cols]
        g, b, h = par[0:1], par[1:2], par[2:3]
        live = stbuf[src, :, cols].astype(jnp.float32)
        u = vf * vt
        gc_bs, gc_mbs = g * cs + b * sn, g * cs - b * sn
        gs_bc, gs_mbc = g * sn + b * cs, g * sn - b * cs
        bh = -(b + h)
        pf = live * (g * vf * vf - u * gc_bs)
        qf = live * (bh * vf * vf - u * gs_mbc)
        pt = live * (g * vt * vt - u * gc_mbs)
        qt = live * (bh * vt * vt + u * gs_bc)
        fd = live * u * (
            quantity(0, 2) * gs_mbc - quantity(0, 3) * gc_bs
            + quantity(1, 2) * gs_bc + quantity(1, 3) * gc_mbs
        )
        flow[src, :, cols] = pf * pf + qf * qf
        blank = [jnp.zeros((ROWS - 3 * per, chunk), jnp.float32)]
        lefts, hots = [], []
        label = lax.broadcasted_iota(jnp.int32, (SPAN, chunk), 0).astype(bf16)
        for end, terms in ((0, [pf, qf, fd]), (1, [pt, qt, -fd])):
            value = jnp.concatenate(terms + blank, axis=0)
            head = value.astype(bf16).astype(jnp.float32)
            both = jnp.concatenate([head, value - head], axis=0).astype(bf16)
            spot = ebuf[src, end : end + 1, cols]
            row = jnp.broadcast_to(spot >> 8, (2 * ROWS, chunk)).astype(bf16)
            low = jnp.broadcast_to((spot & (SPAN - 1)), (2 * ROWS, chunk)).astype(bf16)
            low = jnp.concatenate([low] * (SPAN // (2 * ROWS)), axis=0)
            hots.append(jnp.where(low == label, bf16(1), bf16(0)))
            lefts.append(jnp.concatenate(
                [jnp.where(row == bf16(k), both, bf16(0)) for k in range(high)], axis=0
            ))
        acc[...] += lax.dot_general(
            jnp.concatenate(lefts, axis=1), jnp.concatenate(hots, axis=1),
            (((1,), (1,)), ((), ())), preferred_element_type=jnp.float32,
        )

    final = ranks * pieces - 1

    def one_step(step, picked):
        src = lax.rem(me - step + ranks, ranks)

        @pl.when(step > 0)
        def _():
            remote(params, pbuf.at[me], 3, step).wait()
            remote(status3.at[0], stbuf.at[me], 4, step).wait()

        def advance(t, picked):
            i = step * pieces + t
            following = pick(jnp.minimum(i + 1, final))
            process(i, picked)
            return following

        picked = lax.fori_loop(0, pieces, advance, picked)

        @pl.when(step > 0)
        def _():
            remote(flow.at[src], rflow.at[me], 6, ranks - step).start()

        return picked

    lax.fori_loop(0, ranks, one_step, pick(0))

    for k in range(high):
        at = k * SPAN
        row = k * 2 * ROWS
        sums = acc[row : row + ROWS, :] + acc[row + ROWS : row + 2 * ROWS, :]
        for q in range(3):
            res[at // nb, q, :, at % nb : at % nb + SPAN] = sums[q * per : (q + 1) * per, :]

    back = []
    for step in range(1, ranks):
        peer = lax.rem(me + step, ranks)
        back.append((
            remote(res.at[peer], rbuf.at[me], 5, step),
        ))
    for group in back:
        group[0].start()
    rbuf[me] = res[me]
    rflow[me] = flow[me]
    for step in range(1, ranks):
        remote(flow.at[me], rflow.at[me], 6, step).wait()
    for group in back:
        group[0].wait()

    rate = rating[...] * rating[...]
    for src in range(ranks):
        for s in range(per):
            c = src * per + s
            total = jnp.zeros((1, 1), jnp.float32)
            for k in range(2):
                row = rbuf[src, k, s : s + 1, :] - net[c, k : k + 1, :]
                mis_out[c, k : k + 1, :] = row
                total = total + jnp.sum(row * row, axis=1, keepdims=True)
            sqs[c : c + 1, 0:1] = total
        rows = slice(src * per, (src + 1) * per)
        dual = rbuf[src, 2] + ang[rows, :]
        dual_out[rows, :] = dual
        sqs[rows, 1:2] = jnp.sum(dual * dual, axis=1, keepdims=True)
        lim = status[rows, :].astype(jnp.float32) * (rflow[src] + slack[rows, :] - rate)
        lim_out[rows, :] = lim
        sqs[rows, 2:3] = jnp.sum(lim * lim, axis=1, keepdims=True)

    sqbuf[me] = sqs[...]
    rowbuf[mine] = jnp.sum(sqs[...], axis=0, keepdims=True)
    near = [remote(sqbuf.at[me], sqbuf.at[me], 7, step) for step in range(1, ranks)]
    for copy in near:
        copy.start()

    def begin(i, c):
        all_peers(rowbuf, rowbuf.at[mine], sq_send, sq_recv, i).start()
        return c

    def finish(i, c):
        all_peers(rowbuf, rowbuf.at[mine], sq_send, sq_recv, i).wait()
        return c

    lax.fori_loop(1, count, begin, 0)
    for copy in near:
        copy.wait()
    lax.fori_loop(1, count, finish, 0)

    def add(i, c):
        return c + rowbuf[i]

    zero = jnp.zeros((scen, LANES), jnp.float32)
    group_sum = zero
    for z in range(ranks):
        group_sum = group_sum + sqbuf[z]
    norm_out[...] = jnp.sqrt(group_sum[:, 0:4])
    everything = lax.fori_loop(0, count, add, jnp.zeros((1, LANES), jnp.float32))
    tot_out[...] = jnp.sqrt(everything[:, 0:4] / (scen * groups))


def per_device(
    base_vm, base_va, delta_state, multipliers, net_inj, ang_grad, from_bus, to_bus,
    status, conduct, suscept, charging, rating, slack, zdual,
):
    groups, ranks = lax.axis_size("ctg"), lax.axis_size("br")
    count = groups * ranks
    scen, _, nb = delta_state.shape
    nl = from_bus.shape[0]
    per = scen // ranks
    buses = nb * ranks
    high = buses // SPAN
    base = jnp.stack([base_vm, base_va])
    ends = jnp.stack([from_bus, to_bus])
    params = jnp.stack([conduct, suscept, charging])
    f32 = jnp.float32
    vmem = pl.BlockSpec(memory_space=pltpu.VMEM)
    hbm = pl.BlockSpec(memory_space=pl.ANY)
    mis, dual, lim, norms, tot = pl.pallas_call(
        functools.partial(body, groups, ranks),
        out_shape=(
            jax.ShapeDtypeStruct((scen, 2, nb), f32),
            jax.ShapeDtypeStruct((scen, nb), f32),
            jax.ShapeDtypeStruct((scen, nl), f32),
            jax.ShapeDtypeStruct((scen, 4), f32),
            jax.ShapeDtypeStruct((1, 4), f32),
        ),
        in_specs=[vmem, hbm, hbm, hbm, hbm, vmem, vmem, vmem, vmem, hbm, hbm, hbm],
        out_specs=(vmem,) * 5,
        scratch_shapes=[
            pltpu.VMEM((count, 2, base_vm.shape[0]), f32),
            pltpu.VMEM((ranks, per, 2, nb), f32),
            pltpu.VMEM((ranks, per, 2, nb), f32),
            pltpu.VMEM((ranks, 2, nl), jnp.int32),
            pltpu.VMEM((ranks, 3, nl), f32),
            pltpu.VMEM((ranks, per, nl), jnp.int32),
            pltpu.VMEM((ROWS, buses), f32),
            pltpu.VMEM((high * 2 * ROWS, SPAN), f32),
            pltpu.VMEM((ranks, 3, per, nb), f32),
            pltpu.VMEM((ranks, 3, per, nb), f32),
            pltpu.VMEM((ranks, per, nl), f32),
            pltpu.VMEM((ranks, per, nl), f32),
            pltpu.VMEM((scen, LANES), f32),
            pltpu.VMEM((ranks, scen, LANES), f32),
            pltpu.VMEM((count, 1, LANES), f32),
            pltpu.VMEM((scen, 2, nb), f32),
            pltpu.VMEM((scen, nb), f32),
            pltpu.VMEM((scen, nl), jnp.int32),
            pltpu.VMEM((scen, nl), f32),
            pltpu.VMEM((scen, nl), f32),
            pltpu.SemaphoreType.DMA((7,)),
            pltpu.SemaphoreType.DMA((8, ranks)),
            pltpu.SemaphoreType.DMA((8, ranks)),
            pltpu.SemaphoreType.DMA((count,)),
            pltpu.SemaphoreType.DMA((count,)),
            pltpu.SemaphoreType.DMA((count,)),
            pltpu.SemaphoreType.DMA((count,)),
        ],
        compiler_params=pltpu.CompilerParams(
            collective_id=0, has_side_effects=True, vmem_limit_bytes=48 << 20
        ),
    )(
        base, delta_state, multipliers, net_inj, ang_grad, ends, params, rating[None, :],
        status.reshape(ranks, per, nl), status, slack, zdual,
    )
    return (mis, dual, lim, norms, tot[0])


def solution(mesh):
    placed = (
        P(("ctg", "br")), P(("ctg", "br")),
        P("ctg", None, "br"), P("ctg", None, "br"), P("ctg", None, "br"), P("ctg", "br"),
        P("br"), P("br"), P("ctg", "br"), P("br"), P("br"), P("br"), P("br"),
        P("ctg", "br"), P("ctg", "br"),
    )
    return jax.shard_map(
        per_device,
        mesh=mesh,
        in_specs=placed,
        out_specs=(P("ctg", None, "br"), P("ctg", "br"), P("ctg", "br"), P("ctg", None), P()),
        check_vma=False,
    )
```

```python
import functools

import jax
import jax.numpy as jnp
from jax import lax
from jax.experimental import pallas as pl
from jax.experimental.pallas import tpu as pltpu
from jax.sharding import PartitionSpec as P

LANES = 128
SPAN = 256
ROWS = 8
MESH = pl.DeviceIdType.MESH


def sin_cos(x):
    y = x * x
    sin_c = (1 / 6227020800, -1 / 39916800, 1 / 362880, -1 / 5040, 1 / 120, -1 / 6)
    cos_c = (-1 / 87178291200, 1 / 479001600, -1 / 3628800, 1 / 40320, -1 / 720, 1 / 24, -0.5)
    s = jnp.full_like(y, sin_c[0])
    for c in sin_c[1:]:
        s = s * y + c
    k = jnp.full_like(y, cos_c[0])
    for c in cos_c[1:]:
        k = k * y + c
    return x + x * y * s, 1.0 + y * k


def body(
    groups, ranks,
    base, delta, mult, net_any, ang_any, ends, params, rating, status3, status_any, slack_any, zdual_any,
    mis_out, dual_out, lim_out, norm_out, tot_out,
    bbuf, dbuf, mbuf, ebuf, pbuf, stbuf, table, acc,
    res, rbuf, flow, rflow, sqs, sqbuf, rowbuf,
    net, ang, status, slack, zdual, local,
    send, recv, base_send, base_recv, sq_send, sq_recv,
):
    grp, me = lax.axis_index("ctg"), lax.axis_index("br")
    count = groups * ranks
    mine = grp * ranks + me
    per = dbuf.shape[1]
    nb, nl = delta.shape[2], ends.shape[1]
    scen = delta.shape[0]

    own = pl.ds(me * per, per)
    local_copies = [
        pltpu.make_async_copy(a, b, local.at[i])
        for i, (a, b) in enumerate((
            (delta.at[own], dbuf.at[me]), (mult.at[own], mbuf.at[me]),
            (status_any, status), (slack_any, slack), (zdual_any, zdual),
            (net_any, net), (ang_any, ang),
        ))
    ]
    for copy in local_copies:
        copy.start()

    barrier = pltpu.get_barrier_semaphore()

    def greet(i, carry):
        peer = lax.rem(mine + i, count)
        pl.semaphore_signal(
            barrier, inc=1, device_id=(peer // ranks, lax.rem(peer, ranks)), device_id_type=MESH
        )
        return carry

    lax.fori_loop(1, count, greet, 0)
    pl.semaphore_wait(barrier, count - 1)

    def remote(src, dst, kind, step):
        return pltpu.make_async_remote_copy(
            src_ref=src, dst_ref=dst, send_sem=send.at[kind, step], recv_sem=recv.at[kind, step],
            device_id=(grp, lax.rem(me + step, ranks)), device_id_type=MESH,
        )

    def all_peers(slots, block, sends, recvs, i):
        peer = lax.rem(mine + i, count)
        return pltpu.make_async_remote_copy(
            src_ref=block, dst_ref=slots.at[mine], send_sem=sends.at[i], recv_sem=recvs.at[i],
            device_id=(peer // ranks, lax.rem(peer, ranks)), device_id_type=MESH,
        )

    def begin_base(i, c):
        all_peers(bbuf, base, base_send, base_recv, i).start()
        return c

    def finish_base(i, c):
        all_peers(bbuf, base, base_send, base_recv, i).wait()
        return c

    lax.fori_loop(1, count, begin_base, 0)
    first = []
    for step in range(1, ranks):
        peer = lax.rem(me + step, ranks)
        part = pl.ds(peer * per, per)
        first.append((
            remote(delta.at[part], dbuf.at[me], 0, step),
            remote(mult.at[part], mbuf.at[me], 1, step),
            remote(ends, ebuf.at[me], 2, step),
            remote(params, pbuf.at[me], 3, step),
            remote(status3.at[peer], stbuf.at[me], 4, step),
        ))
    for kind in range(5):
        for group in first:
            group[kind].start()

    bbuf[mine] = base[...]
    ebuf[me] = ends[...]
    pbuf[me] = params[...]
    stbuf[me] = status3[me]
    table[...] = jnp.zeros_like(table)
    acc[...] = jnp.zeros_like(acc)
    sqs[...] = jnp.zeros_like(sqs)
    for copy in local_copies:
        copy.wait()
    live_own = status[...].astype(jnp.float32)
    comp = live_own * (zdual[...] * slack[...] - 0.01)
    sqs[:, 3:4] = jnp.sum(comp * comp, axis=1, keepdims=True)

    lax.fori_loop(1, count, finish_base, 0)
    for group in first:
        for copy in group[:3]:
            copy.wait()

    for src in range(ranks):
        cols = slice(src * nb, (src + 1) * nb)
        volts = jnp.concatenate([bbuf[src * groups + i] for i in range(groups)], axis=1)
        for s in range(per):
            table[s : s + 1, cols] = volts[0:1] + dbuf[src, s, 0:1, :]
            table[per + s : per + s + 1, cols] = volts[1:2] + dbuf[src, s, 1:2, :]
            table[2 * per + s : 2 * per + s + 1, cols] = mbuf[src, s, 0:1, :]
            table[3 * per + s : 3 * per + s + 1, cols] = mbuf[src, s, 1:2, :]

    tiles = table.shape[1] // LANES
    high = table.shape[1] // SPAN

    chunk = SPAN if nl % SPAN == 0 else LANES
    pieces = nl // chunk
    bf16 = jnp.bfloat16

    def place(i):
        return lax.rem(me - i // pieces + ranks, ranks), pl.ds(pl.multiple_of(lax.rem(i, pieces) * chunk, chunk), chunk)

    def pick(i):
        src, cols = place(i)
        picked = []
        for end in range(2):
            spots = jnp.broadcast_to(ebuf[src, end : end + 1, cols], (ROWS, chunk))
            tiles_found = []
            for at in range(0, chunk, LANES):
                spot = spots[:, at : at + LANES]
                low, tile = spot & (LANES - 1), spot >> 7
                found = jnp.zeros((ROWS, LANES), jnp.float32)
                for k in range(tiles):
                    piece = jnp.take_along_axis(
                        table[:, k * LANES : (k + 1) * LANES], low, axis=1, mode="promise_in_bounds"
                    )
                    found = jnp.where(tile == k, piece, found)
                tiles_found.append(found)
            picked.append(jnp.concatenate(tiles_found, axis=1))
        return tuple(picked)

    def process(i, picked):
        src, cols = place(i)

        def quantity(end, q):
            return picked[end][q * per : (q + 1) * per, :]

        vf, vt = quantity(0, 0), quantity(1, 0)
        sn, cs = sin_cos(quantity(0, 1) - quantity(1, 1))
        par = pbuf[src, :, cols]
        g, b, h = par[0:1], par[1:2], par[2:3]
        live = stbuf[src, :, cols].astype(jnp.float32)
        u = vf * vt
        gc_bs, gc_mbs = g * cs + b * sn, g * cs - b * sn
        gs_bc, gs_mbc = g * sn + b * cs, g * sn - b * cs
        bh = -(b + h)
        pf = live * (g * vf * vf - u * gc_bs)
        qf = live * (bh * vf * vf - u * gs_mbc)
        pt = live * (g * vt * vt - u * gc_mbs)
        qt = live * (bh * vt * vt + u * gs_bc)
        fd = live * u * (
            quantity(0, 2) * gs_mbc - quantity(0, 3) * gc_bs
            + quantity(1, 2) * gs_bc + quantity(1, 3) * gc_mbs
        )
        flow[src, :, cols] = pf * pf + qf * qf
        blank = [jnp.zeros((ROWS - 3 * per, chunk), jnp.float32)]
        lefts, hots = [], []
        label = lax.broadcasted_iota(jnp.int32, (SPAN, chunk), 0).astype(bf16)
        for end, terms in ((0, [pf, qf, fd]), (1, [pt, qt, -fd])):
            value = jnp.concatenate(terms + blank, axis=0)
            head = value.astype(bf16).astype(jnp.float32)
            both = jnp.concatenate([head, value - head], axis=0).astype(bf16)
            spot = ebuf[src, end : end + 1, cols]
            row = jnp.broadcast_to(spot >> 8, (2 * ROWS, chunk)).astype(bf16)
            low = jnp.broadcast_to((spot & (SPAN - 1)), (2 * ROWS, chunk)).astype(bf16)
            low = jnp.concatenate([low] * (SPAN // (2 * ROWS)), axis=0)
            hots.append(jnp.where(low == label, bf16(1), bf16(0)))
            lefts.append(jnp.concatenate(
                [jnp.where(row == bf16(k), both, bf16(0)) for k in range(high)], axis=0
            ))
        acc[...] += lax.dot_general(
            jnp.concatenate(lefts, axis=1), jnp.concatenate(hots, axis=1),
            (((1,), (1,)), ((), ())), preferred_element_type=jnp.float32,
        )

    final = ranks * pieces - 1

    def one_step(step, picked):
        src = lax.rem(me - step + ranks, ranks)

        @pl.when(step > 0)
        def _():
            remote(params, pbuf.at[me], 3, step).wait()
            remote(status3.at[0], stbuf.at[me], 4, step).wait()

        def advance(t, picked):
            i = step * pieces + t
            following = pick(jnp.minimum(i + 1, final))
            process(i, picked)
            return following

        picked = lax.fori_loop(0, pieces, advance, picked)

        @pl.when(step > 0)
        def _():
            remote(flow.at[src], rflow.at[me], 6, ranks - step).start()

        return picked

    lax.fori_loop(0, ranks, one_step, pick(0))

    for k in range(high):
        at = k * SPAN
        row = k * 2 * ROWS
        sums = acc[row : row + ROWS, :] + acc[row + ROWS : row + 2 * ROWS, :]
        for q in range(3):
            res[at // nb, q, :, at % nb : at % nb + SPAN] = sums[q * per : (q + 1) * per, :]

    back = []
    for step in range(1, ranks):
        peer = lax.rem(me + step, ranks)
        back.append((
            remote(res.at[peer], rbuf.at[me], 5, step),
        ))
    for group in back:
        group[0].start()
    rbuf[me] = res[me]
    rflow[me] = flow[me]
    for step in range(1, ranks):
        remote(flow.at[me], rflow.at[me], 6, step).wait()
    for group in back:
        group[0].wait()

    rate = rating[...] * rating[...]
    for src in range(ranks):
        for s in range(per):
            c = src * per + s
            total = jnp.zeros((1, 1), jnp.float32)
            for k in range(2):
                row = rbuf[src, k, s : s + 1, :] - net[c, k : k + 1, :]
                mis_out[c, k : k + 1, :] = row
                total = total + jnp.sum(row * row, axis=1, keepdims=True)
            sqs[c : c + 1, 0:1] = total
        rows = slice(src * per, (src + 1) * per)
        dual = rbuf[src, 2] + ang[rows, :]
        dual_out[rows, :] = dual
        sqs[rows, 1:2] = jnp.sum(dual * dual, axis=1, keepdims=True)
        lim = status[rows, :].astype(jnp.float32) * (rflow[src] + slack[rows, :] - rate)
        lim_out[rows, :] = lim
        sqs[rows, 2:3] = jnp.sum(lim * lim, axis=1, keepdims=True)

    sqbuf[me] = sqs[...]
    near = [remote(sqbuf.at[me], sqbuf.at[me], 7, step) for step in range(1, ranks)]
    for copy in near:
        copy.start()
    for copy in near:
        copy.wait()
    group_sum = jnp.zeros((scen, LANES), jnp.float32)
    for z in range(ranks):
        group_sum = group_sum + sqbuf[z]
    norm_out[...] = jnp.sqrt(group_sum[:, 0:4])

    rowbuf[grp] = jnp.sum(group_sum, axis=0, keepdims=True)

    def across(i):
        return pltpu.make_async_remote_copy(
            src_ref=rowbuf.at[grp], dst_ref=rowbuf.at[grp],
            send_sem=sq_send.at[i], recv_sem=sq_recv.at[i],
            device_id=(lax.rem(grp + i, groups), me), device_id_type=MESH,
        )

    def begin(i, c):
        across(i).start()
        return c

    def finish(i, c):
        across(i).wait()
        return c

    lax.fori_loop(1, groups, begin, 0)
    lax.fori_loop(1, groups, finish, 0)

    def add(i, c):
        return c + rowbuf[i]

    everything = lax.fori_loop(0, groups, add, jnp.zeros((1, LANES), jnp.float32))
    tot_out[...] = jnp.sqrt(everything[:, 0:4] / (scen * groups))


def per_device(
    base_vm, base_va, delta_state, multipliers, net_inj, ang_grad, from_bus, to_bus,
    status, conduct, suscept, charging, rating, slack, zdual,
):
    groups, ranks = lax.axis_size("ctg"), lax.axis_size("br")
    count = groups * ranks
    scen, _, nb = delta_state.shape
    nl = from_bus.shape[0]
    per = scen // ranks
    buses = nb * ranks
    high = buses // SPAN
    base = jnp.stack([base_vm, base_va])
    ends = jnp.stack([from_bus, to_bus])
    params = jnp.stack([conduct, suscept, charging])
    f32 = jnp.float32
    vmem = pl.BlockSpec(memory_space=pltpu.VMEM)
    hbm = pl.BlockSpec(memory_space=pl.ANY)
    mis, dual, lim, norms, tot = pl.pallas_call(
        functools.partial(body, groups, ranks),
        out_shape=(
            jax.ShapeDtypeStruct((scen, 2, nb), f32),
            jax.ShapeDtypeStruct((scen, nb), f32),
            jax.ShapeDtypeStruct((scen, nl), f32),
            jax.ShapeDtypeStruct((scen, 4), f32),
            jax.ShapeDtypeStruct((1, 4), f32),
        ),
        in_specs=[vmem, hbm, hbm, hbm, hbm, vmem, vmem, vmem, vmem, hbm, hbm, hbm],
        out_specs=(vmem,) * 5,
        scratch_shapes=[
            pltpu.VMEM((count, 2, base_vm.shape[0]), f32),
            pltpu.VMEM((ranks, per, 2, nb), f32),
            pltpu.VMEM((ranks, per, 2, nb), f32),
            pltpu.VMEM((ranks, 2, nl), jnp.int32),
            pltpu.VMEM((ranks, 3, nl), f32),
            pltpu.VMEM((ranks, per, nl), jnp.int32),
            pltpu.VMEM((ROWS, buses), f32),
            pltpu.VMEM((high * 2 * ROWS, SPAN), f32),
            pltpu.VMEM((ranks, 3, per, nb), f32),
            pltpu.VMEM((ranks, 3, per, nb), f32),
            pltpu.VMEM((ranks, per, nl), f32),
            pltpu.VMEM((ranks, per, nl), f32),
            pltpu.VMEM((scen, LANES), f32),
            pltpu.VMEM((ranks, scen, LANES), f32),
            pltpu.VMEM((groups, 1, LANES), f32),
            pltpu.VMEM((scen, 2, nb), f32),
            pltpu.VMEM((scen, nb), f32),
            pltpu.VMEM((scen, nl), jnp.int32),
            pltpu.VMEM((scen, nl), f32),
            pltpu.VMEM((scen, nl), f32),
            pltpu.SemaphoreType.DMA((7,)),
            pltpu.SemaphoreType.DMA((8, ranks)),
            pltpu.SemaphoreType.DMA((8, ranks)),
            pltpu.SemaphoreType.DMA((count,)),
            pltpu.SemaphoreType.DMA((count,)),
            pltpu.SemaphoreType.DMA((count,)),
            pltpu.SemaphoreType.DMA((count,)),
        ],
        compiler_params=pltpu.CompilerParams(
            collective_id=0, has_side_effects=True, vmem_limit_bytes=48 << 20
        ),
    )(
        base, delta_state, multipliers, net_inj, ang_grad, ends, params, rating[None, :],
        status.reshape(ranks, per, nl), status, slack, zdual,
    )
    return (mis, dual, lim, norms, tot[0])


def solution(mesh):
    placed = (
        P(("ctg", "br")), P(("ctg", "br")),
        P("ctg", None, "br"), P("ctg", None, "br"), P("ctg", None, "br"), P("ctg", "br"),
        P("br"), P("br"), P("ctg", "br"), P("br"), P("br"), P("br"), P("br"),
        P("ctg", "br"), P("ctg", "br"),
    )
    return jax.shard_map(
        per_device,
        mesh=mesh,
        in_specs=placed,
        out_specs=(P("ctg", None, "br"), P("ctg", "br"), P("ctg", "br"), P("ctg", None), P()),
        check_vma=False,
    )
```
